32 devices in a mesh: expert: 4 (over z), shard: 8 (over y, x, core).
Axes of the slice: x: 2, y: 2, z: 4, core: 2. Of those that a mesh axis runs over, the one named last changes fastest.
Arguments:
- master_down: float32 [16, 6400, 4096], P('expert', None, 'shard'), may hold values from -0.109375 to 0.109375
- second_down: bfloat16 [16, 6400, 4096], P('expert', None, 'shard'), may hold values from -0.0390625 to 0.0390625
- router_weight: float32 [4096, 16], P('shard', 'expert'), may hold values from -0.09375 to 0.09375
- router_gain: float32 [4096], P('shard'), may hold values from 0.25 to 1.75
Outputs:
- final_down: bfloat16 [16, 6400, 4096], P('expert', 'shard')
- scale_down: float32 [16, 6400], P('expert', 'shard')
- serve_router: bfloat16 [4096, 16], replicated
The draws below stay inside these ranges and needn't reach their ends.
All inputs are finite; a program needn't handle non-finite values.
Results may differ from the reference program's by a relative error of at most 0.001.
Values may be sent and summed in bfloat16 or wider, within the bound.
A program may use at most 256 MiB of HBM per device.

```python
import jax
import jax.numpy as jnp
from jax import lax

EXPERTS = 16
D_MODEL = 4096
D_EXPERT = 6400


def spiked(values, stream_key, source, target, blocks, factor):
    def block_of(position):
        return (jnp.arange(values.shape[position]) // (values.shape[position] // blocks)).reshape((-1,) + (1,) * (values.ndim - 1 - position))

    one_side = jax.random.permutation(stream_key, blocks)[block_of(target)]
    other_side = (block_of(target) + blocks // 2) % blocks
    return jnp.where((block_of(source) == one_side) | (block_of(source) == other_side), factor * values, values)


def level_of(key, shape, split, low, top_value):
    loudness, own = 1.0, jax.random.fold_in(key, 6)
    for position, parts in split:
        draws = jnp.exp(jax.random.uniform(jax.random.fold_in(own, position), (parts,), jnp.float32, low / len(split), top_value / len(split)))
        loudness = loudness * jnp.repeat(draws, shape[position] // parts).reshape([-1 if axis == position else 1 for axis in range(len(shape))])
    return loudness


def bell_draw(key, shape, width, most, shards=(), kind=jnp.bfloat16):
    entries = width * jax.random.normal(key, shape, jnp.float32)
    if shards:
        entries = entries * level_of(key, shape, shards, -0.22, 0.18)
    return jnp.clip(entries, -most, most).astype(kind)


def bell_draw_with(rng, shape, scale, most, split, heavy, dtype=jnp.bfloat16):
    array = scale * jax.random.normal(rng, shape, jnp.float32)
    if split:
        array = array * level_of(rng, shape, split, -0.22, 0.18)
    return jnp.clip(spiked(array, jax.random.fold_in(rng, 3), *heavy), -most, most).astype(dtype)


def setup_inputs(seed: int = 0) -> dict:
    splits = jax.random.split(jax.random.key(seed), 5)
    return {
        "master_down": bell_draw_with(splits[0], (EXPERTS, D_EXPERT, D_MODEL), D_EXPERT ** -0.5, 0.109375, ((0, 4), (2, 8)), (2, 1, 8, 2.0), jnp.float32),
        "second_down": bell_draw(splits[1], (EXPERTS, D_EXPERT, D_MODEL), (D_EXPERT * 4) ** -0.5, 0.0390625, ((0, 4), (2, 8))),
        "router_weight": bell_draw(splits[2], (D_MODEL, EXPERTS), D_MODEL ** -0.5, 0.09375, ((0, 8), (1, 4)), jnp.float32),
        "router_gain": jnp.clip(1.0 + 0.15 * jax.random.normal(splits[3], (D_MODEL,), jnp.float32), 0.25, 1.75),
    }


def reference(master_down, second_down, router_weight, router_gain):
    merged_down = master_down + second_down.astype(jnp.float32)
    scale_down = jnp.sqrt(lax.optimization_barrier(jnp.sum(merged_down * merged_down, axis=2)))
    final_down = (merged_down / jnp.expand_dims(scale_down, 2)).astype(jnp.bfloat16)
    serve_router = (router_weight * router_gain[:, None]).astype(jnp.bfloat16)
    return (final_down, scale_down, serve_router)
```

```python
import functools

import jax
import jax.numpy as jnp
from jax import lax
from jax.experimental import pallas as pl
from jax.experimental.pallas import tpu as pltpu
from jax.sharding import PartitionSpec as P

MESH = pl.DeviceIdType.MESH
QUEUE = 3
READS = 3
DIRECT = 2
GROUP = 16
LANES = 128


def rows_per_chunk(rows):
    return max(r for r in range(16, 129, 16) if rows % r == 0)


def flipped(index, mask):
    out, bit = 0, 1
    while bit <= mask:
        own = lax.rem(index // bit, 2)
        if mask & bit:
            out = out + bit * (1 - 2 * own)
        bit *= 2
    return index + out


def kernel(
    shards, groups, master, second, weight, gain,
    final, scale, router,
    sum_master, sum_second, norm_master, norm_second, ready,
    part, landed, total, early, rpart, rall,
    sum_sems, norm_sems, send_sems, own_sems, final_sems,
    part_send, part_recv, total_send, total_recv, early_send, early_recv,
    rsend, rrecv, gsend, grecv, weight_here, gain_here, small_sems, own,
):
    experts, _, rows, cols = master.shape
    take = rows_per_chunk(rows)
    blocks = rows // take
    chunks = experts * blocks
    bits = shards.bit_length() - 1
    lag = bits + 1
    per = LANES // GROUP
    parts = take // GROUP
    lines = shards * take // LANES
    me = lax.axis_index("shard")
    group = lax.axis_index("expert")
    parity = lax.rem(me, 2)

    barrier = pltpu.get_barrier_semaphore()
    for o in range(shards - 1, 0, -1):
        pl.semaphore_signal(barrier, inc=1, device_id={"shard": flipped(me, o)}, device_id_type=MESH)
    for o in range(1, groups):
        pl.semaphore_signal(barrier, inc=1, device_id={"expert": lax.rem(group + o, groups)}, device_id_type=MESH)

    def reads(k, bufs, sems):
        slot = lax.rem(k, READS)
        e, b = k // blocks, lax.rem(k, blocks)
        where = pl.ds(pl.multiple_of(b * take, 16), take)
        return [
            pltpu.make_async_copy(src.at[e, :, where, :], buf.at[slot], sems.at[i, slot])
            for i, (src, buf) in enumerate(zip((master, second), bufs))
        ]

    sum_bufs, norm_bufs = (sum_master, sum_second), (norm_master, norm_second)

    for k in range(min(READS, chunks)):
        for c in reads(k, sum_bufs, sum_sems):
            c.start()
    small = [
        pltpu.make_async_copy(weight, weight_here, small_sems.at[0]),
        pltpu.make_async_copy(gain, gain_here, small_sems.at[1]),
    ]
    for c in small:
        c.start()
    for k in range(min(READS, chunks)):
        for c in reads(k, norm_bufs, norm_sems):
            c.start()

    mine = pl.ds(pl.multiple_of(me * cols, 128), cols)

    shift = lax.broadcasted_iota(jnp.int32, (GROUP, LANES), 1) - lax.broadcasted_iota(jnp.int32, (GROUP, LANES), 0)

    def place(j):
        d, i = j // parts, lax.rem(j, parts)
        return d, pl.ds(pl.multiple_of(i * GROUP, GROUP), GROUP)

    def row_sums(k, dst):
        slot = lax.rem(k, READS)
        for c in reads(k, sum_bufs, sum_sems):
            c.wait()

        def one(s, carry):
            acc = jnp.zeros((GROUP, LANES), jnp.float32)
            for m in range(per):
                d, where = place(s * per + m)
                x = sum_master[slot, d, where, :] + sum_second[slot, d, where, :].astype(jnp.float32)
                column = jnp.sum(x * x, axis=1, keepdims=True)
                acc = acc + jnp.where(shift == GROUP * m, column, 0.0)
            dst[s] = jnp.sum(acc, axis=0, keepdims=True)
            return carry

        lax.fori_loop(0, lines, one, 0)

        @pl.when(k + READS < chunks)
        def _():
            for c in reads(k + READS, sum_bufs, sum_sems):
                c.start()

    def early_copy(k, o):
        return pltpu.make_async_remote_copy(
            src_ref=early.at[k, me],
            dst_ref=early.at[k, me],
            send_sem=early_send.at[k],
            recv_sem=early_recv.at[k, me],
            device_id={"shard": flipped(me, o)},
            device_id_type=MESH,
        )

    def exchange(stage, k):
        return pltpu.make_async_remote_copy(
            src_ref=part.at[stage, k],
            dst_ref=landed.at[stage, k],
            send_sem=part_send.at[stage],
            recv_sem=part_recv.at[stage, k],
            device_id={"shard": flipped(me, 1 << stage)},
            device_id_type=MESH,
        )

    def hand_over(k):
        return pltpu.make_async_remote_copy(
            src_ref=total.at[k],
            dst_ref=total.at[k],
            send_sem=total_send,
            recv_sem=total_recv.at[k],
            device_id={"shard": flipped(me, 1)},
            device_id_type=MESH,
        )

    def send(k, o):
        slot = lax.rem(k, QUEUE)
        e, b = k // blocks, lax.rem(k, blocks)
        where = pl.ds(pl.multiple_of(b * take, 16), take)
        to = flipped(me, o)
        return pltpu.make_async_remote_copy(
            src_ref=ready.at[slot, to],
            dst_ref=final.at[e, where, mine],
            send_sem=send_sems.at[slot],
            recv_sem=final_sems.at[me],
            device_id={"shard": to},
            device_id_type=MESH,
        )

    def keep(k):
        slot = lax.rem(k, QUEUE)
        e, b = k // blocks, lax.rem(k, blocks)
        where = pl.ds(pl.multiple_of(b * take, 16), take)
        return pltpu.make_async_copy(ready.at[slot, me], final.at[e, where, mine], own_sems.at[slot])

    def drain(k):
        slot = lax.rem(k, QUEUE)
        several = ready.at[slot, pl.ds(0, shards - 1)]
        pltpu.make_async_copy(several, several, send_sems.at[slot]).wait()
        keep(k).wait()

    def normalise(k):
        slot = lax.rem(k, READS)
        out = lax.rem(k, QUEUE)
        for c in reads(k, norm_bufs, norm_sems):
            c.wait()

        @pl.when(k >= QUEUE)
        def _():
            drain(k - QUEUE)

        def one(s, carry):
            line = 1.0 / jnp.sqrt(total[k, s])
            for m in range(per):
                d, where = place(s * per + m)
                column = jnp.sum(jnp.where(shift == GROUP * m, line, 0.0), axis=1, keepdims=True)
                x = norm_master[slot, d, where, :] + norm_second[slot, d, where, :].astype(jnp.float32)
                ready[out, d, where, :] = (x * column).astype(jnp.bfloat16)
            return carry

        lax.fori_loop(0, lines, one, 0)

        @pl.when(k + READS < chunks)
        def _():
            for c in reads(k + READS, norm_bufs, norm_sems):
                c.start()

        for o in range(shards - 1, 0, -1):
            send(k, o).start()
        keep(k).start()

    first = min(DIRECT, chunks)
    row_sums(0, early.at[0, me])
    pl.semaphore_wait(barrier, shards + groups - 2)
    for k in range(first):
        if k:
            row_sums(k, early.at[k, me])
        for o in range(shards - 1, 0, -1):
            early_copy(k, o).start()

    for c in small:
        c.wait()
    product = (weight_here[...] * gain_here[...]).astype(jnp.bfloat16)
    rpart[...] = product
    rall[group, :, mine] = product

    def rows_copy(o):
        return pltpu.make_async_remote_copy(
            src_ref=rpart,
            dst_ref=rall.at[group, :, mine],
            send_sem=rsend,
            recv_sem=rrecv.at[me],
            device_id={"shard": flipped(me, o)},
            device_id_type=MESH,
        )

    for o in range(1, shards):
        rows_copy(o).start()

    def tick(t, carry):
        @pl.when(t < chunks)
        def _():
            row_sums(t, part.at[0, t])

            @pl.when(lax.rem(t, 2) != parity)
            def _():
                exchange(0, t).start()

        n = t - lag

        @pl.when((n >= 0) & (n < first))
        def _():
            for o in range(1, shards):
                other = flipped(me, o)
                pltpu.make_async_copy(early.at[n, other], early.at[n, other], early_recv.at[n, other]).wait()
            sums = early[n, 0]
            for s in range(1, shards):
                sums = sums + early[n, s]
            total[n] = sums

        @pl.when((n >= first) & (lax.rem(n, 2) != parity))
        def _():
            hand_over(n).wait_recv()

        @pl.when(n >= 0)
        def _():
            normalise(n)

        for stage in range(bits):
            k = t - 1 - stage

            @pl.when((k >= first) & (k < chunks) & (lax.rem(k, 2) == parity))
            def _():
                exchange(stage, k).wait_recv()
                if stage + 1 < bits:
                    part[stage + 1, k] = part[stage, k] + landed[stage, k]
                    exchange(stage + 1, k).start()
                else:
                    total[k] = part[stage, k] + landed[stage, k]
                    hand_over(k).start()

        return carry

    lax.fori_loop(first, chunks + lag, tick, 0)

    def group_copy(o):
        return pltpu.make_async_remote_copy(
            src_ref=rall.at[group],
            dst_ref=rall.at[group],
            send_sem=gsend.at[o],
            recv_sem=grecv.at[group],
            device_id={"expert": lax.rem(group + o, groups)},
            device_id_type=MESH,
        )

    for o in range(1, shards):
        rows_copy(o).wait_send()
        other = flipped(me, o)
        there = rall.at[group, :, pl.ds(pl.multiple_of(other * cols, 128), cols)]
        pltpu.make_async_copy(there, there, rrecv.at[other]).wait()
    for o in range(1, groups):
        group_copy(o).start()

    here = rows // GROUP

    def own_lines(e, carry):
        for line in range(-(-here // per)):
            acc = jnp.zeros((GROUP, LANES), jnp.float32)
            for m in range(min(per, here - line * per)):
                b, i = divmod(line * per + m, parts)
                j = me * parts + i
                source = total[e * blocks + b, j // per]
                column = jnp.sum(jnp.where(shift == GROUP * lax.rem(j, per), source, 0.0), axis=1, keepdims=True)
                acc = acc + jnp.where(shift == GROUP * m, column, 0.0)
            own[e, :, line * LANES : (line + 1) * LANES] = jnp.sqrt(jnp.sum(acc, axis=0, keepdims=True))
        return carry

    lax.fori_loop(0, experts, own_lines, 0)
    for e in range(experts):
        scale[e : e + 1, :] = own[e, :, :rows]

    for o in range(1, groups):
        other = lax.rem(group + o, groups)
        pltpu.make_async_copy(rall.at[other], rall.at[other], grecv.at[other]).wait()
        group_copy(o).wait_send()
    gcols = weight.shape[0]
    spot = lax.broadcasted_iota(jnp.int32, router.shape, 0)
    table = jnp.zeros(router.shape, jnp.float32)
    for g in range(groups):
        block = rall[g].astype(jnp.float32)
        for c in range(gcols):
            table = jnp.where(spot == g * gcols + c, block[c : c + 1, :], table)
    router[...] = table.astype(jnp.bfloat16)

    for k in range(first):
        several = early.at[k, pl.ds(0, shards - 1)]
        pltpu.make_async_copy(several, several, early_send.at[k]).wait()

    def settle(k, carry):
        @pl.when(lax.rem(k, 2) != parity)
        def _():
            exchange(0, k).wait_send()

        @pl.when(lax.rem(k, 2) == parity)
        def _():
            for stage in range(1, bits):
                exchange(stage, k).wait_send()
            hand_over(k).wait_send()

        return carry

    lax.fori_loop(first, chunks, settle, 0)
    for k in range(max(0, chunks - QUEUE), chunks):
        drain(k)
    for o in range(1, shards):
        other = flipped(me, o)
        there = final.at[:, :, pl.ds(pl.multiple_of(other * cols, 128), cols)]
        pltpu.make_async_copy(there, there, final_sems.at[other]).wait()


def write_out(final, scale, router, final_out, scale_out, router_out, sems):
    experts = final.shape[0]
    copies = [
        pltpu.make_async_copy(scale, scale_out, sems.at[experts]),
        pltpu.make_async_copy(router, router_out, sems.at[experts + 1]),
    ]
    copies += [pltpu.make_async_copy(final.at[e], final_out.at[e], sems.at[e]) for e in range(experts)]
    for c in copies:
        c.start()
    for c in copies:
        c.wait()


def local(shards, groups, master_down, second_down, router_weight, router_gain):
    experts, d_expert, cols = master_down.shape
    rows = d_expert // shards
    take = rows_per_chunk(rows)
    chunks = experts * (rows // take)
    bits = shards.bit_length() - 1
    lines = shards * take // LANES
    gcols = router_weight.shape[1]
    f32, bf16 = jnp.float32, jnp.bfloat16
    first = min(DIRECT, chunks)
    shapes = (
        jax.ShapeDtypeStruct((experts, rows, cols * shards), bf16),
        jax.ShapeDtypeStruct((experts, rows), f32),
        jax.ShapeDtypeStruct((groups * gcols, cols * shards), bf16),
    )
    in_vmem = pl.BlockSpec(memory_space=pltpu.VMEM)
    in_hbm = pl.BlockSpec(memory_space=pltpu.HBM)
    anywhere = pl.BlockSpec(memory_space=pl.ANY)
    dma = pltpu.SemaphoreType.DMA
    inside = pl.pallas_call(
        functools.partial(kernel, shards, groups),
        out_shape=shapes,
        in_specs=[anywhere] * 2 + [in_hbm] * 2,
        out_specs=(in_vmem,) * 3,
        scratch_shapes=[
            pltpu.VMEM((READS, shards, take, cols), f32),
            pltpu.VMEM((READS, shards, take, cols), bf16),
            pltpu.VMEM((READS, shards, take, cols), f32),
            pltpu.VMEM((READS, shards, take, cols), bf16),
            pltpu.VMEM((QUEUE, shards, take, cols), bf16),
            pltpu.VMEM((bits, chunks, lines, 1, LANES), f32),
            pltpu.VMEM((bits, chunks, lines, 1, LANES), f32),
            pltpu.VMEM((chunks, lines, 1, LANES), f32),
            pltpu.VMEM((first, shards, lines, 1, LANES), f32),
            pltpu.VMEM((gcols, cols), bf16),
            pltpu.VMEM((groups, gcols, cols * shards), bf16),
            dma((2, READS)),
            dma((2, READS)),
            dma((QUEUE,)),
            dma((QUEUE,)),
            dma((shards,)),
            dma((bits,)),
            dma((bits, chunks)),
            dma,
            dma((chunks,)),
            dma((first,)),
            dma((first, shards)),
            dma,
            dma((shards,)),
            dma((groups,)),
            dma((groups,)),
            pltpu.VMEM((gcols, cols), f32),
            pltpu.VMEM((1, cols), f32),
            dma((2,)),
            pltpu.VMEM((experts, 1, -(-rows // LANES) * LANES), f32),
        ],
        compiler_params=pltpu.CompilerParams(collective_id=0, has_side_effects=True, vmem_limit_bytes=28 * 2**20),
    )(
        master_down.reshape(experts, shards, rows, cols),
        second_down.reshape(experts, shards, rows, cols),
        pltpu.with_memory_space_constraint(router_weight.T, pltpu.HBM),
        pltpu.with_memory_space_constraint(router_gain[None, :], pltpu.HBM),
    )
    final, scale, router = pl.pallas_call(
        write_out,
        out_shape=shapes,
        in_specs=[in_vmem] * 3,
        out_specs=(in_hbm,) * 3,
        scratch_shapes=[dma((experts + 2,))],
        compiler_params=pltpu.CompilerParams(vmem_limit_bytes=2**20),
    )(*inside)
    return (final, scale, router.T)


def solution(mesh):
    shards, groups = mesh.shape["shard"], mesh.shape["expert"]
    return jax.shard_map(
        functools.partial(local, shards, groups),
        mesh=mesh,
        in_specs=(
            P("expert", None, "shard"),
            P("expert", None, "shard"),
            P("shard", "expert"),
            P("shard"),
        ),
        out_specs=(P("expert", "shard", None), P("expert", "shard"), P()),
        check_vma=False,
    )
```

```python
import functools

import jax
import jax.numpy as jnp
from jax import lax
from jax.experimental import pallas as pl
from jax.experimental.pallas import tpu as pltpu
from jax.sharding import PartitionSpec as P

MESH = pl.DeviceIdType.MESH
QUEUE = 3
READS = 3
DIRECT = 2
RING = 8
GROUP = 16
LANES = 128


def rows_per_chunk(rows):
    return max(r for r in range(16, 129, 16) if rows % r == 0)


def flipped(index, mask):
    out, bit = 0, 1
    while bit <= mask:
        own = lax.rem(index // bit, 2)
        if mask & bit:
            out = out + bit * (1 - 2 * own)
        bit *= 2
    return index + out


def crossed(index, mask, bits):
    out, bit = 0, 1
    for _ in range(bits):
        a, b = lax.rem(index // bit, 2), lax.rem(mask // bit, 2)
        out = out + bit * (a + b - 2 * a * b)
        bit *= 2
    return out


def kernel(
    shards, groups, master, second, weight, gain,
    final, scale, router,
    sum_master, sum_second, norm_master, norm_second, ready,
    part, landed, total, early, rpart, rall,
    sum_sems, norm_sems, send_sems, own_sems, final_sems,
    part_send, part_recv, total_send, total_recv, early_send, early_recv,
    rsend, rrecv, gsend, grecv, weight_here, gain_here, small_sems, own, inverse,
):
    experts, _, rows, cols = master.shape
    take = rows_per_chunk(rows)
    blocks = rows // take
    chunks = experts * blocks
    bits = shards.bit_length() - 1
    lag = bits + 1
    per = LANES // GROUP
    parts = take // GROUP
    lines = shards * take // LANES
    me = lax.axis_index("shard")
    group = lax.axis_index("expert")
    parity = lax.rem(me, 2)

    barrier = pltpu.get_barrier_semaphore()
    for o in range(shards - 1, 0, -1):
        pl.semaphore_signal(barrier, inc=1, device_id={"shard": flipped(me, o)}, device_id_type=MESH)
    for o in range(1, groups):
        pl.semaphore_signal(barrier, inc=1, device_id={"expert": lax.rem(group + o, groups)}, device_id_type=MESH)

    def reads(k, bufs, sems):
        slot = lax.rem(k, READS)
        e, b = k // blocks, lax.rem(k, blocks)
        where = pl.ds(pl.multiple_of(b * take, 16), take)
        return [
            pltpu.make_async_copy(src.at[e, :, where, :], buf.at[slot], sems.at[i, slot])
            for i, (src, buf) in enumerate(zip((master, second), bufs))
        ]

    sum_bufs, norm_bufs = (sum_master, sum_second), (norm_master, norm_second)

    for k in range(min(READS, chunks)):
        for c in reads(k, sum_bufs, sum_sems):
            c.start()
    small = [
        pltpu.make_async_copy(weight, weight_here, small_sems.at[0]),
        pltpu.make_async_copy(gain, gain_here, small_sems.at[1]),
    ]
    for c in small:
        c.start()
    for k in range(min(READS, chunks)):
        for c in reads(k, norm_bufs, norm_sems):
            c.start()

    mine = pl.ds(pl.multiple_of(me * cols, 128), cols)

    shift = lax.broadcasted_iota(jnp.int32, (GROUP, LANES), 1) - lax.broadcasted_iota(jnp.int32, (GROUP, LANES), 0)

    def place(j):
        d, i = j // parts, lax.rem(j, parts)
        return d, pl.ds(pl.multiple_of(i * GROUP, GROUP), GROUP)

    def row_sums(k, dst):
        slot = lax.rem(k, READS)
        for c in reads(k, sum_bufs, sum_sems):
            c.wait()

        def one(s, carry):
            acc = jnp.zeros((GROUP, LANES), jnp.float32)
            for m in range(per):
                d, where = place(s * per + m)
                x = sum_master[slot, d, where, :] + sum_second[slot, d, where, :].astype(jnp.float32)
                column = jnp.sum(x * x, axis=1, keepdims=True)
                acc = acc + jnp.where(shift == GROUP * m, column, 0.0)
            dst[s] = jnp.sum(acc, axis=0, keepdims=True)
            return carry

        lax.fori_loop(0, lines, one, 0)

        @pl.when(k + READS < chunks)
        def _():
            for c in reads(k + READS, sum_bufs, sum_sems):
                c.start()

    def early_copy(k, o):
        return pltpu.make_async_remote_copy(
            src_ref=early.at[k, me],
            dst_ref=early.at[k, me],
            send_sem=early_send.at[k],
            recv_sem=early_recv.at[k],
            device_id={"shard": flipped(me, o)},
            device_id_type=MESH,
        )

    def exchange(stage, k):
        return pltpu.make_async_remote_copy(
            src_ref=part.at[stage, k],
            dst_ref=landed.at[stage, k],
            send_sem=part_send.at[stage],
            recv_sem=part_recv.at[stage, lax.rem(k, RING)],
            device_id={"shard": flipped(me, 1 << stage)},
            device_id_type=MESH,
        )

    def hand_over(k):
        return pltpu.make_async_remote_copy(
            src_ref=total.at[k],
            dst_ref=total.at[k],
            send_sem=total_send,
            recv_sem=total_recv.at[lax.rem(k, RING)],
            device_id={"shard": flipped(me, 1)},
            device_id_type=MESH,
        )

    def send(k, to):
        slot = lax.rem(k, QUEUE)
        e, b = k // blocks, lax.rem(k, blocks)
        where = pl.ds(pl.multiple_of(b * take, 16), take)
        return pltpu.make_async_remote_copy(
            src_ref=ready.at[slot, to],
            dst_ref=final.at[e, where, mine],
            send_sem=send_sems.at[slot],
            recv_sem=final_sems.at[me],
            device_id={"shard": to},
            device_id_type=MESH,
        )

    def keep(k):
        slot = lax.rem(k, QUEUE)
        e, b = k // blocks, lax.rem(k, blocks)
        where = pl.ds(pl.multiple_of(b * take, 16), take)
        return pltpu.make_async_copy(ready.at[slot, me], final.at[e, where, mine], own_sems.at[slot])

    def drain(k):
        slot = lax.rem(k, QUEUE)
        several = ready.at[slot, pl.ds(0, shards - 1)]
        pltpu.make_async_copy(several, several, send_sems.at[slot]).wait()
        keep(k).wait()

    def normalise(k):
        slot = lax.rem(k, READS)
        out = lax.rem(k, QUEUE)
        for c in reads(k, norm_bufs, norm_sems):
            c.wait()

        @pl.when(k >= QUEUE)
        def _():
            drain(k - QUEUE)

        inverse[...] = 1.0 / jnp.sqrt(total[k])

        def one(i, carry):
            to = crossed(me, shards - 1 - i, bits)
            for p in range(parts):
                j = to * parts + p
                where = pl.ds(p * GROUP, GROUP)
                line = jnp.where(shift == GROUP * lax.rem(j, per), inverse[j // per], 0.0)
                column = jnp.sum(line, axis=1, keepdims=True)
                x = norm_master[slot, to, where, :] + norm_second[slot, to, where, :].astype(jnp.float32)
                ready[out, to, where, :] = (x * column).astype(jnp.bfloat16)

            @pl.when(i < shards - 1)
            def _():
                send(k, to).start()

            return carry

        lax.fori_loop(0, shards, one, 0)
        keep(k).start()

        @pl.when(k + READS < chunks)
        def _():
            for c in reads(k + READS, norm_bufs, norm_sems):
                c.start()

    first = min(DIRECT, chunks)
    row_sums(0, early.at[0, me])
    pl.semaphore_wait(barrier, shards + groups - 2)
    for k in range(first):
        if k:
            row_sums(k, early.at[k, me])
        for o in range(shards - 1, 0, -1):
            early_copy(k, o).start()

    for c in small:
        c.wait()
    product = (weight_here[...] * gain_here[...]).astype(jnp.bfloat16)
    rpart[...] = product
    rall[group, :, mine] = product

    def rows_copy(o):
        return pltpu.make_async_remote_copy(
            src_ref=rpart,
            dst_ref=rall.at[group, :, mine],
            send_sem=rsend,
            recv_sem=rrecv,
            device_id={"shard": flipped(me, o)},
            device_id_type=MESH,
        )

    for o in range(1, shards):
        rows_copy(o).start()

    def tick(t, carry):
        @pl.when(t < chunks)
        def _():
            row_sums(t, part.at[0, t])

            @pl.when(lax.rem(t, 2) != parity)
            def _():
                exchange(0, t).start()

        n = t - lag

        @pl.when((n >= 0) & (n < first))
        def _():
            several = early.at[n, pl.ds(0, shards - 1)]
            pltpu.make_async_copy(several, several, early_recv.at[n]).wait()
            sums = early[n, 0]
            for s in range(1, shards):
                sums = sums + early[n, s]
            total[n] = sums

        @pl.when((n >= first) & (lax.rem(n, 2) != parity))
        def _():
            hand_over(n).wait_recv()

        @pl.when(n >= 0)
        def _():
            normalise(n)

        for stage in range(bits):
            k = t - 1 - stage

            @pl.when((k >= first) & (k < chunks) & (lax.rem(k, 2) == parity))
            def _():
                exchange(stage, k).wait_recv()
                if stage + 1 < bits:
                    part[stage + 1, k] = part[stage, k] + landed[stage, k]
                    exchange(stage + 1, k).start()
                else:
                    total[k] = part[stage, k] + landed[stage, k]
                    hand_over(k).start()

        return carry

    lax.fori_loop(first, chunks + lag, tick, 0)

    def group_copy(o):
        return pltpu.make_async_remote_copy(
            src_ref=rall.at[group],
            dst_ref=rall.at[group],
            send_sem=gsend,
            recv_sem=grecv,
            device_id={"expert": lax.rem(group + o, groups)},
            device_id_type=MESH,
        )

    for o in range(1, shards):
        rows_copy(o).wait_send()
    several = rall.at[group, :, pl.ds(0, (shards - 1) * cols)]
    pltpu.make_async_copy(several, several, rrecv).wait()
    for o in range(1, groups):
        group_copy(o).start()

    here = rows // GROUP

    def own_lines(e, carry):
        for line in range(-(-here // per)):
            acc = jnp.zeros((GROUP, LANES), jnp.float32)
            for m in range(min(per, here - line * per)):
                b, i = divmod(line * per + m, parts)
                j = me * parts + i
                source = total[e * blocks + b, j // per]
                column = jnp.sum(jnp.where(shift == GROUP * lax.rem(j, per), source, 0.0), axis=1, keepdims=True)
                acc = acc + jnp.where(shift == GROUP * m, column, 0.0)
            own[e, :, line * LANES : (line + 1) * LANES] = jnp.sqrt(jnp.sum(acc, axis=0, keepdims=True))
        return carry

    lax.fori_loop(0, experts, own_lines, 0)
    for e in range(experts):
        scale[e : e + 1, :] = own[e, :, :rows]

    for o in range(1, groups):
        group_copy(o).wait_send()
    several = rall.at[pl.ds(0, groups - 1)]
    pltpu.make_async_copy(several, several, grecv).wait()
    gcols = weight.shape[0]
    spot = lax.broadcasted_iota(jnp.int32, router.shape, 0)
    table = jnp.zeros(router.shape, jnp.float32)
    for g in range(groups):
        block = rall[g].astype(jnp.float32)
        for c in range(gcols):
            table = jnp.where(spot == g * gcols + c, block[c : c + 1, :], table)
    router[...] = table.astype(jnp.bfloat16)

    for k in range(first):
        several = early.at[k, pl.ds(0, shards - 1)]
        pltpu.make_async_copy(several, several, early_send.at[k]).wait()

    def settle(k, carry):
        @pl.when(lax.rem(k, 2) != parity)
        def _():
            exchange(0, k).wait_send()

        @pl.when(lax.rem(k, 2) == parity)
        def _():
            for stage in range(1, bits):
                exchange(stage, k).wait_send()
            hand_over(k).wait_send()

        return carry

    lax.fori_loop(first, chunks, settle, 0)
    for k in range(max(0, chunks - QUEUE), chunks):
        drain(k)
    for o in range(1, shards):
        other = flipped(me, o)
        there = final.at[:, :, pl.ds(pl.multiple_of(other * cols, 128), cols)]
        pltpu.make_async_copy(there, there, final_sems.at[other]).wait()


def write_out(final, scale, router, final_out, scale_out, router_out, sems):
    experts = final.shape[0]
    copies = [
        pltpu.make_async_copy(scale, scale_out, sems.at[experts]),
        pltpu.make_async_copy(router, router_out, sems.at[experts + 1]),
    ]
    copies += [pltpu.make_async_copy(final.at[e], final_out.at[e], sems.at[e]) for e in range(experts)]
    for c in copies:
        c.start()
    for c in copies:
        c.wait()


def local(shards, groups, master_down, second_down, router_weight, router_gain):
    experts, d_expert, cols = master_down.shape
    rows = d_expert // shards
    take = rows_per_chunk(rows)
    chunks = experts * (rows // take)
    bits = shards.bit_length() - 1
    lines = shards * take // LANES
    gcols = router_weight.shape[1]
    f32, bf16 = jnp.float32, jnp.bfloat16
    first = min(DIRECT, chunks)
    shapes = (
        jax.ShapeDtypeStruct((experts, rows, cols * shards), bf16),
        jax.ShapeDtypeStruct((experts, rows), f32),
        jax.ShapeDtypeStruct((groups * gcols, cols * shards), bf16),
    )
    in_vmem = pl.BlockSpec(memory_space=pltpu.VMEM)
    in_hbm = pl.BlockSpec(memory_space=pltpu.HBM)
    anywhere = pl.BlockSpec(memory_space=pl.ANY)
    dma = pltpu.SemaphoreType.DMA
    inside = pl.pallas_call(
        functools.partial(kernel, shards, groups),
        out_shape=shapes,
        in_specs=[anywhere] * 2 + [in_hbm] * 2,
        out_specs=(in_vmem,) * 3,
        scratch_shapes=[
            pltpu.VMEM((READS, shards, take, cols), f32),
            pltpu.VMEM((READS, shards, take, cols), bf16),
            pltpu.VMEM((READS, shards, take, cols), f32),
            pltpu.VMEM((READS, shards, take, cols), bf16),
            pltpu.VMEM((QUEUE, shards, take, cols), bf16),
            pltpu.VMEM((bits, chunks, lines, 1, LANES), f32),
            pltpu.VMEM((bits, chunks, lines, 1, LANES), f32),
            pltpu.VMEM((chunks, lines, 1, LANES), f32),
            pltpu.VMEM((first, shards, lines, 1, LANES), f32),
            pltpu.VMEM((gcols, cols), bf16),
            pltpu.VMEM((groups, gcols, cols * shards), bf16),
            dma((2, READS)),
            dma((2, READS)),
            dma((QUEUE,)),
            dma((QUEUE,)),
            dma((shards,)),
            dma((bits,)),
            dma((bits, RING)),
            dma,
            dma((RING,)),
            dma((first,)),
            dma((first,)),
            dma,
            dma,
            dma,
            dma,
            pltpu.VMEM((gcols, cols), f32),
            pltpu.VMEM((1, cols), f32),
            dma((2,)),
            pltpu.VMEM((experts, 1, -(-rows // LANES) * LANES), f32),
            pltpu.VMEM((lines, 1, LANES), f32),
        ],
        compiler_params=pltpu.CompilerParams(collective_id=0, has_side_effects=True, vmem_limit_bytes=28 * 2**20),
    )(
        master_down.reshape(experts, shards, rows, cols),
        second_down.reshape(experts, shards, rows, cols),
        pltpu.with_memory_space_constraint(router_weight.T, pltpu.HBM),
        pltpu.with_memory_space_constraint(router_gain[None, :], pltpu.HBM),
    )
    final, scale, router = pl.pallas_call(
        write_out,
        out_shape=shapes,
        in_specs=[in_vmem] * 3,
        out_specs=(in_hbm,) * 3,
        scratch_shapes=[dma((experts + 2,))],
        compiler_params=pltpu.CompilerParams(vmem_limit_bytes=2**20),
    )(*inside)
    return (final, scale, router.T)


def solution(mesh):
    shards, groups = mesh.shape["shard"], mesh.shape["expert"]
    return jax.shard_map(
        functools.partial(local, shards, groups),
        mesh=mesh,
        in_specs=(
            P("expert", None, "shard"),
            P("expert", None, "shard"),
            P("shard", "expert"),
            P("shard"),
        ),
        out_specs=(P("expert", "shard", None), P("expert", "shard"), P()),
        check_vma=False,
    )
```

```python
import functools

import jax
import jax.numpy as jnp
from jax import lax
from jax.experimental import pallas as pl
from jax.experimental.pallas import tpu as pltpu
from jax.sharding import PartitionSpec as P

MESH = pl.DeviceIdType.MESH
QUEUE = 3
READS = 3
DIRECT = 2
RING = 8
GROUP = 16
LANES = 128


def rows_per_chunk(rows):
    return max(r for r in range(16, 129, 16) if rows % r == 0)


def flipped(index, mask):
    out, bit = 0, 1
    while bit <= mask:
        own = lax.rem(index // bit, 2)
        if mask & bit:
            out = out + bit * (1 - 2 * own)
        bit *= 2
    return index + out


def crossed(index, mask, bits):
    out, bit = 0, 1
    for _ in range(bits):
        a, b = lax.rem(index // bit, 2), lax.rem(mask // bit, 2)
        out = out + bit * (a + b - 2 * a * b)
        bit *= 2
    return out


def kernel(
    shards, groups, master, second, weight, gain,
    final, scale, router,
    sum_master, sum_second, norm_master, norm_second, ready,
    part, landed, total, early, rpart, rall,
    sum_sems, norm_sems, send_sems, own_sems, final_sems,
    part_send, part_recv, total_send, total_recv, early_send, early_recv,
    rsend, rrecv, gsend, grecv, weight_here, gain_here, small_sems, own, inverse, raw, raw_in, raw_send, raw_recv,
):
    experts, _, rows, cols = master.shape
    take = rows_per_chunk(rows)
    blocks = rows // take
    chunks = experts * blocks
    bits = shards.bit_length() - 1
    lag = bits + 1
    per = LANES // GROUP
    parts = take // GROUP
    lines = shards * take // LANES
    me = lax.axis_index("shard")
    group = lax.axis_index("expert")
    parity = lax.rem(me, 2)

    barrier = pltpu.get_barrier_semaphore()
    for o in range(shards - 1, 0, -1):
        pl.semaphore_signal(barrier, inc=1, device_id={"shard": flipped(me, o)}, device_id_type=MESH)
    for o in range(1, groups):
        pl.semaphore_signal(barrier, inc=1, device_id={"expert": lax.rem(group + o, groups)}, device_id_type=MESH)

    def reads(k, bufs, sems):
        slot = lax.rem(k, READS)
        e, b = k // blocks, lax.rem(k, blocks)
        where = pl.ds(pl.multiple_of(b * take, 16), take)
        return [
            pltpu.make_async_copy(src.at[e, :, where, :], buf.at[slot], sems.at[i, slot])
            for i, (src, buf) in enumerate(zip((master, second), bufs))
        ]

    sum_bufs, norm_bufs = (sum_master, sum_second), (norm_master, norm_second)

    for k in range(min(READS, chunks)):
        for c in reads(k, sum_bufs, sum_sems):
            c.start()
    small = [
        pltpu.make_async_copy(weight, weight_here, small_sems.at[0]),
        pltpu.make_async_copy(gain, gain_here, small_sems.at[1]),
    ]
    for c in small:
        c.start()
    for k in range(min(READS, chunks)):
        for c in reads(k, norm_bufs, norm_sems):
            c.start()

    mine = pl.ds(pl.multiple_of(me * cols, 128), cols)

    shift = lax.broadcasted_iota(jnp.int32, (GROUP, LANES), 1) - lax.broadcasted_iota(jnp.int32, (GROUP, LANES), 0)

    def place(j):
        d, i = j // parts, lax.rem(j, parts)
        return d, pl.ds(pl.multiple_of(i * GROUP, GROUP), GROUP)

    def row_sums(k, dst, copied=False):
        slot = lax.rem(k, READS)
        for c in reads(k, sum_bufs, sum_sems):
            c.wait()

        def one(s, carry):
            acc = jnp.zeros((GROUP, LANES), jnp.float32)
            for m in range(per):
                d, where = place(s * per + m)
                x = sum_master[slot, d, where, :] + sum_second[slot, d, where, :].astype(jnp.float32)
                column = jnp.sum(x * x, axis=1, keepdims=True)
                acc = acc + jnp.where(shift == GROUP * m, column, 0.0)
            dst[s] = jnp.sum(acc, axis=0, keepdims=True)
            return carry

        lax.fori_loop(0, lines, one, 0)
        if copied:
            for d in range(shards):
                raw[d] = sum_master[slot, d, :GROUP, :] + sum_second[slot, d, :GROUP, :].astype(jnp.float32)

        @pl.when(k + READS < chunks)
        def _():
            for c in reads(k + READS, sum_bufs, sum_sems):
                c.start()

    def early_copy(k, o):
        return pltpu.make_async_remote_copy(
            src_ref=early.at[k, me],
            dst_ref=early.at[k, me],
            send_sem=early_send.at[k],
            recv_sem=early_recv.at[k],
            device_id={"shard": flipped(me, o)},
            device_id_type=MESH,
        )

    def raw_copy(o):
        to = flipped(me, o)
        return pltpu.make_async_remote_copy(
            src_ref=raw.at[to],
            dst_ref=raw_in.at[me],
            send_sem=raw_send,
            recv_sem=raw_recv,
            device_id={"shard": to},
            device_id_type=MESH,
        )

    def exchange(stage, k):
        return pltpu.make_async_remote_copy(
            src_ref=part.at[stage, k],
            dst_ref=landed.at[stage, k],
            send_sem=part_send.at[stage],
            recv_sem=part_recv.at[stage, lax.rem(k, RING)],
            device_id={"shard": flipped(me, 1 << stage)},
            device_id_type=MESH,
        )

    def hand_over(k):
        return pltpu.make_async_remote_copy(
            src_ref=total.at[k],
            dst_ref=total.at[k],
            send_sem=total_send,
            recv_sem=total_recv.at[lax.rem(k, RING)],
            device_id={"shard": flipped(me, 1)},
            device_id_type=MESH,
        )

    def send(k, to):
        slot = lax.rem(k, QUEUE)
        e, b = k // blocks, lax.rem(k, blocks)
        where = pl.ds(pl.multiple_of(b * take, 16), take)
        return pltpu.make_async_remote_copy(
            src_ref=ready.at[slot, to],
            dst_ref=final.at[e, where, mine],
            send_sem=send_sems.at[slot],
            recv_sem=final_sems.at[e],
            device_id={"shard": to},
            device_id_type=MESH,
        )

    def send_rest(to):
        return pltpu.make_async_remote_copy(
            src_ref=ready.at[0, to, pl.ds(GROUP, take - GROUP)],
            dst_ref=final.at[0, pl.ds(GROUP, take - GROUP), mine],
            send_sem=send_sems.at[0],
            recv_sem=final_sems.at[0],
            device_id={"shard": to},
            device_id_type=MESH,
        )

    def keep(k):
        slot = lax.rem(k, QUEUE)
        e, b = k // blocks, lax.rem(k, blocks)
        where = pl.ds(pl.multiple_of(b * take, 16), take)
        return pltpu.make_async_copy(ready.at[slot, me], final.at[e, where, mine], own_sems.at[slot])

    def drain(k):
        slot = lax.rem(k, QUEUE)


        @pl.when(k > 0)
        def _():
            several = ready.at[slot, pl.ds(0, shards - 1)]
            pltpu.make_async_copy(several, several, send_sems.at[slot]).wait()

        @pl.when(k == 0)
        def _():
            several = ready.at[0, pl.ds(0, shards - 1), pl.ds(GROUP, take - GROUP)]
            pltpu.make_async_copy(several, several, send_sems.at[0]).wait()

        keep(k).wait()

    def normalise(k):
        slot = lax.rem(k, READS)
        out = lax.rem(k, QUEUE)
        for c in reads(k, norm_bufs, norm_sems):
            c.wait()

        @pl.when(k >= QUEUE)
        def _():
            drain(k - QUEUE)

        inverse[...] = 1.0 / jnp.sqrt(total[k])

        def one(i, carry):
            to = crossed(me, shards - 1 - i, bits)
            for p in range(parts):
                j = to * parts + p
                where = pl.ds(p * GROUP, GROUP)
                line = jnp.where(shift == GROUP * lax.rem(j, per), inverse[j // per], 0.0)
                column = jnp.sum(line, axis=1, keepdims=True)
                x = norm_master[slot, to, where, :] + norm_second[slot, to, where, :].astype(jnp.float32)
                ready[out, to, where, :] = (x * column).astype(jnp.bfloat16)

            @pl.when((i < shards - 1) & (k > 0))
            def _():
                send(k, to).start()

            @pl.when((i < shards - 1) & (k == 0))
            def _():
                send_rest(to).start()

            return carry

        lax.fori_loop(0, shards, one, 0)
        keep(k).start()

        @pl.when(k + READS < chunks)
        def _():
            for c in reads(k + READS, norm_bufs, norm_sems):
                c.start()

    first = min(DIRECT, chunks)
    row_sums(0, early.at[0, me], copied=True)
    pl.semaphore_wait(barrier, shards + groups - 2)
    for k in range(first):
        if k:
            row_sums(k, early.at[k, me])
        for o in range(shards - 1, 0, -1):
            early_copy(k, o).start()
        if k == 0:
            for o in range(shards - 1, 0, -1):
                raw_copy(o).start()

    for c in small:
        c.wait()
    product = (weight_here[...] * gain_here[...]).astype(jnp.bfloat16)
    rpart[...] = product
    rall[group, :, mine] = product

    def rows_copy(o):
        return pltpu.make_async_remote_copy(
            src_ref=rpart,
            dst_ref=rall.at[group, :, mine],
            send_sem=rsend,
            recv_sem=rrecv,
            device_id={"shard": flipped(me, o)},
            device_id_type=MESH,
        )

    for o in range(1, shards):
        rows_copy(o).start()

    def tick(t, carry):
        @pl.when(t < chunks)
        def _():
            row_sums(t, part.at[0, t])

            @pl.when(lax.rem(t, 2) != parity)
            def _():
                exchange(0, t).start()

        n = t - lag

        @pl.when((n >= 0) & (n < first))
        def _():
            several = early.at[n, pl.ds(0, shards - 1)]
            pltpu.make_async_copy(several, several, early_recv.at[n]).wait()
            sums = early[n, 0]
            for s in range(1, shards):
                sums = sums + early[n, s]
            total[n] = sums

        @pl.when((n >= first) & (lax.rem(n, 2) != parity))
        def _():
            hand_over(n).wait_recv()

        @pl.when(n >= 0)
        def _():
            normalise(n)

        for stage in range(bits):
            k = t - 1 - stage

            @pl.when((k >= first) & (k < chunks) & (lax.rem(k, 2) == parity))
            def _():
                exchange(stage, k).wait_recv()
                if stage + 1 < bits:
                    part[stage + 1, k] = part[stage, k] + landed[stage, k]
                    exchange(stage + 1, k).start()
                else:
                    total[k] = part[stage, k] + landed[stage, k]
                    hand_over(k).start()

        return carry

    lax.fori_loop(first, chunks + lag, tick, 0)

    def group_copy(o):
        return pltpu.make_async_remote_copy(
            src_ref=rall.at[group],
            dst_ref=rall.at[group],
            send_sem=gsend,
            recv_sem=grecv,
            device_id={"expert": lax.rem(group + o, groups)},
            device_id_type=MESH,
        )

    for o in range(1, shards):
        rows_copy(o).wait_send()
    several = rall.at[group, :, pl.ds(0, (shards - 1) * cols)]
    pltpu.make_async_copy(several, several, rrecv).wait()
    for o in range(1, groups):
        group_copy(o).start()

    here = rows // GROUP

    def own_lines(e, carry):
        for line in range(-(-here // per)):
            acc = jnp.zeros((GROUP, LANES), jnp.float32)
            for m in range(min(per, here - line * per)):
                b, i = divmod(line * per + m, parts)
                j = me * parts + i
                source = total[e * blocks + b, j // per]
                column = jnp.sum(jnp.where(shift == GROUP * lax.rem(j, per), source, 0.0), axis=1, keepdims=True)
                acc = acc + jnp.where(shift == GROUP * m, column, 0.0)
            own[e, :, line * LANES : (line + 1) * LANES] = jnp.sqrt(jnp.sum(acc, axis=0, keepdims=True))
        return carry

    lax.fori_loop(0, experts, own_lines, 0)
    for e in range(experts):
        scale[e : e + 1, :] = own[e, :, :rows]

    for o in range(1, groups):
        group_copy(o).wait_send()
    several = rall.at[pl.ds(0, groups - 1)]
    pltpu.make_async_copy(several, several, grecv).wait()
    gcols = weight.shape[0]
    spot = lax.broadcasted_iota(jnp.int32, router.shape, 0)
    table = jnp.zeros(router.shape, jnp.float32)
    for g in range(groups):
        block = rall[g].astype(jnp.float32)
        for c in range(gcols):
            table = jnp.where(spot == g * gcols + c, block[c : c + 1, :], table)
    router[...] = table.astype(jnp.bfloat16)

    several = raw_in.at[pl.ds(0, shards - 1)]
    pltpu.make_async_copy(several, several, raw_recv).wait()
    pltpu.make_async_copy(several, several, raw_send).wait()
    j = me * parts
    line = jnp.where(shift == GROUP * lax.rem(j, per), 1.0 / jnp.sqrt(total[0, j // per]), 0.0)
    column = jnp.sum(line, axis=1, keepdims=True)
    for d in range(shards):

        @pl.when(me != d)
        def _():
            final[0, :GROUP, d * cols : (d + 1) * cols] = (raw_in[d] * column).astype(jnp.bfloat16)

    for k in range(first):
        several = early.at[k, pl.ds(0, shards - 1)]
        pltpu.make_async_copy(several, several, early_send.at[k]).wait()

    def settle(k, carry):
        @pl.when(lax.rem(k, 2) != parity)
        def _():
            exchange(0, k).wait_send()

        @pl.when(lax.rem(k, 2) == parity)
        def _():
            for stage in range(1, bits):
                exchange(stage, k).wait_send()
            hand_over(k).wait_send()

        return carry

    lax.fori_loop(first, chunks, settle, 0)
    for k in range(max(0, chunks - QUEUE), chunks):
        drain(k)
    for e in range(experts):
        start = 0 if e else GROUP
        there = final.at[e, pl.ds(start, rows - start), pl.ds(0, (shards - 1) * cols)]
        pltpu.make_async_copy(there, there, final_sems.at[e]).wait()


def write_out(final, scale, router, final_out, scale_out, router_out, sems):
    experts = final.shape[0]
    copies = [
        pltpu.make_async_copy(scale, scale_out, sems.at[experts]),
        pltpu.make_async_copy(router, router_out, sems.at[experts + 1]),
    ]
    copies += [pltpu.make_async_copy(final.at[e], final_out.at[e], sems.at[e]) for e in range(experts)]
    for c in copies:
        c.start()
    for c in copies:
        c.wait()


def local(shards, groups, master_down, second_down, router_weight, router_gain):
    experts, d_expert, cols = master_down.shape
    rows = d_expert // shards
    take = rows_per_chunk(rows)
    chunks = experts * (rows // take)
    bits = shards.bit_length() - 1
    lines = shards * take // LANES
    gcols = router_weight.shape[1]
    f32, bf16 = jnp.float32, jnp.bfloat16
    first = min(DIRECT, chunks)
    shapes = (
        jax.ShapeDtypeStruct((experts, rows, cols * shards), bf16),
        jax.ShapeDtypeStruct((experts, rows), f32),
        jax.ShapeDtypeStruct((groups * gcols, cols * shards), bf16),
    )
    in_vmem = pl.BlockSpec(memory_space=pltpu.VMEM)
    in_hbm = pl.BlockSpec(memory_space=pltpu.HBM)
    anywhere = pl.BlockSpec(memory_space=pl.ANY)
    dma = pltpu.SemaphoreType.DMA
    inside = pl.pallas_call(
        functools.partial(kernel, shards, groups),
        out_shape=shapes,
        in_specs=[anywhere] * 2 + [in_hbm] * 2,
        out_specs=(in_vmem,) * 3,
        scratch_shapes=[
            pltpu.VMEM((READS, shards, take, cols), f32),
            pltpu.VMEM((READS, shards, take, cols), bf16),
            pltpu.VMEM((READS, shards, take, cols), f32),
            pltpu.VMEM((READS, shards, take, cols), bf16),
            pltpu.VMEM((QUEUE, shards, take, cols), bf16),
            pltpu.VMEM((bits, chunks, lines, 1, LANES), f32),
            pltpu.VMEM((bits, chunks, lines, 1, LANES), f32),
            pltpu.VMEM((chunks, lines, 1, LANES), f32),
            pltpu.VMEM((first, shards, lines, 1, LANES), f32),
            pltpu.VMEM((gcols, cols), bf16),
            pltpu.VMEM((groups, gcols, cols * shards), bf16),
            dma((2, READS)),
            dma((2, READS)),
            dma((QUEUE,)),
            dma((QUEUE,)),
            dma((experts,)),
            dma((bits,)),
            dma((bits, RING)),
            dma,
            dma((RING,)),
            dma((first,)),
            dma((first,)),
            dma,
            dma,
            dma,
            dma,
            pltpu.VMEM((gcols, cols), f32),
            pltpu.VMEM((1, cols), f32),
            dma((2,)),
            pltpu.VMEM((experts, 1, -(-rows // LANES) * LANES), f32),
            pltpu.VMEM((lines, 1, LANES), f32),
            pltpu.VMEM((shards, GROUP, cols), f32),
            pltpu.VMEM((shards, GROUP, cols), f32),
            dma,
            dma,
        ],
        compiler_params=pltpu.CompilerParams(collective_id=0, has_side_effects=True, vmem_limit_bytes=28 * 2**20),
    )(
        master_down.reshape(experts, shards, rows, cols),
        second_down.reshape(experts, shards, rows, cols),
        pltpu.with_memory_space_constraint(router_weight.T, pltpu.HBM),
        pltpu.with_memory_space_constraint(router_gain[None, :], pltpu.HBM),
    )
    final, scale, router = pl.pallas_call(
        write_out,
        out_shape=shapes,
        in_specs=[in_vmem] * 3,
        out_specs=(in_hbm,) * 3,
        scratch_shapes=[dma((experts + 2,))],
        compiler_params=pltpu.CompilerParams(vmem_limit_bytes=2**20),
    )(*inside)
    return (final, scale, router.T)


def solution(mesh):
    shards, groups = mesh.shape["shard"], mesh.shape["expert"]
    return jax.shard_map(
        functools.partial(local, shards, groups),
        mesh=mesh,
        in_specs=(
            P("expert", None, "shard"),
            P("expert", None, "shard"),
            P("shard", "expert"),
            P("shard"),
        ),
        out_specs=(P("expert", "shard", None), P("expert", "shard"), P()),
        check_vma=False,
    )
```
